32 devices in a mesh: dp: 8 (over y, x, core), mp: 4 (over z).
Axes of the slice: x: 2, y: 2, z: 4, core: 2. Of those that a mesh axis runs over, the one named last changes fastest.
Arguments:
- token_ids: int32 [16], replicated, may hold values from 0 to 3071
- cache_lengths: int32 [16], P('dp'), may hold values from 1 to 512
- embedding: bfloat16 [3072, 12288], P(('dp', 'mp')), may hold values from -6 to 6
- ln_gain: float32 [12288], replicated, may hold values from 0.25 to 1.75
- query_weight: bfloat16 [12288, 6144], P('dp', 'mp'), may hold values from -0.0546875 to 0.0546875
- key_cache: bfloat16 [16, 512, 6144], P('dp', None, 'mp'), may hold values from -1000 to 1000
- value_cache: bfloat16 [16, 512, 6144], P('dp', None, 'mp'), may hold values from -6 to 6
- out_weight: bfloat16 [6144, 12288], P('mp', 'dp'), may hold values from -0.078125 to 0.078125
- final_gain: float32 [12288], replicated, may hold values from 0.25 to 1.75
Outputs:
- log_probs: float32 [16, 3072], P(None, ('dp', 'mp'))
The draws below stay inside these ranges and needn't reach their ends.
All inputs are finite; a program needn't handle non-finite values.
Results may differ from the reference program's by a relative error of at most 0.00033.
Values may be sent and summed in bfloat16 or wider, within the bound.
A program may use at most 128 MiB of HBM per device.

```python
import math
import jax
import jax.numpy as jnp
import numpy as np
from jax import lax

D = 12288
HEADS = 48
HD = 128
CACHE = 512
HQ = 6144
SEQS = 16
VOCAB = 3072


def draw_key_cache(key, part):
    noise_key, dir_key, str_key, pick_key, pos_key = jax.random.split(jax.random.fold_in(key, 7), 5)
    base_noise = jnp.clip(jax.random.normal(noise_key, (SEQS, CACHE, HQ), jnp.float32), -6.0, 6.0)
    lowest = 100.0
    highest = 180.0
    share_of = 0.5
    direction = jnp.clip(jax.random.normal(dir_key, (SEQS, HQ), jnp.float32), -3.0, 3.0)
    strength = lowest * (highest / lowest) ** jax.random.uniform(str_key, (SEQS,), jnp.float32)
    chosen = (jax.random.uniform(pick_key, (SEQS,), jnp.float32) < share_of).astype(jnp.float32)
    position = jax.random.randint(pos_key, (SEQS,), 0, CACHE // 4)
    slot_index = jnp.arange(CACHE)[None, :]
    at_first = (slot_index == position[:, None])[:, :, None]
    at_second = (slot_index == position[:, None] + 1)[:, :, None]
    first_row = jnp.sum(jnp.where(at_first, base_noise, 0.0), axis=1) + (chosen * strength)[:, None] * direction
    planted = jnp.where(at_first, first_row[:, None, :], base_noise)
    planted = jnp.where(at_second, (1.012 * first_row)[:, None, :], planted)
    return planted.astype(jnp.bfloat16)


def set_ends(values, key, least, largest):
    index_at = [jax.random.randint(jax.random.fold_in(key, axis), (), 0, length) for axis, length in enumerate(values.shape)]
    longest = values.shape.index(max(values.shape))
    next_to = index_at[:longest] + [(index_at[longest] + 1) % values.shape[longest]] + index_at[longest + 1:]
    return values.at[tuple(index_at)].set(least).at[tuple(next_to)].set(largest)


def block_scale(stream_key, shape, pieces, smallest, high):
    level, own = 1.0, jax.random.fold_in(stream_key, 6)
    for dim, blocks in pieces:
        steps = jnp.exp(jax.random.uniform(jax.random.fold_in(own, dim), (blocks,), jnp.float32, smallest / len(pieces), high / len(pieces)))
        level = level * jnp.repeat(steps, shape[dim] // blocks).reshape([-1 if axis == dim else 1 for axis in range(len(shape))])
    return level


def cumulative_ranks(amount, skew):
    portions = [(1 << 20) // math.isqrt(rank ** skew) + 1 for rank in range(1, amount + 1)]
    spread = 1 + sum(portions) // (1 << 30)
    return np.cumsum(np.array([max(1, weight // spread) for weight in portions]))


def ranked_ids(rng, dims, amount, slope):
    listing = cumulative_ranks(amount, slope)
    ticket = jax.random.randint(jax.random.fold_in(rng, 1), dims, 0, int(listing[amount - 1]))
    grade = jnp.searchsorted(jnp.asarray(listing, jnp.int32), ticket, side="right")
    return jax.random.permutation(jax.random.fold_in(rng, 2), amount)[grade].astype(jnp.int32)


def normal_values(rng, extent, width, bound, shards=(), kind=jnp.bfloat16):
    drawn = width * jax.random.normal(rng, extent, jnp.float32)
    if shards:
        drawn = drawn * block_scale(rng, extent, shards, -0.22, 0.18)
    return jnp.clip(drawn, -bound, bound).astype(kind)


def setup_inputs(seed: int = 0) -> dict:
    seeds = jax.random.split(jax.random.key(seed), 10)
    token_ids = set_ends(ranked_ids(seeds[0], (SEQS,), VOCAB, 2), jax.random.fold_in(seeds[0], 3), 0, VOCAB - 1).astype(jnp.int32)
    cache_lengths = set_ends(jax.random.randint(seeds[1], (SEQS,), 1, CACHE + 1), jax.random.fold_in(seeds[1], 1), 1, CACHE).astype(jnp.int32)
    embedding = normal_values(seeds[2], (VOCAB, D), 1.0, 6.0, ((0, 32),))
    ln_gain = jnp.clip(1.0 + 0.15 * jax.random.normal(seeds[3], (D,), jnp.float32), 0.25, 1.75)
    query_weight = normal_values(seeds[4], (D, HQ), D ** -0.5, 0.0546875, ((0, 8), (1, 4)))
    key_cache = draw_key_cache(jax.random.fold_in(seeds[9], 71), 0)
    value_cache = normal_values(seeds[6], (SEQS, CACHE, HQ), 1.0, 6.0, ((0, 8), (2, 4)))
    out_weight = normal_values(seeds[7], (HQ, D), HQ ** -0.5, 0.078125, ((0, 4), (1, 8)))
    final_gain = jnp.clip(1.0 + 0.15 * jax.random.normal(seeds[8], (D,), jnp.float32), 0.25, 1.75)
    return {"token_ids": token_ids, "cache_lengths": cache_lengths, "embedding": embedding, "ln_gain": ln_gain, "query_weight": query_weight, "key_cache": key_cache, "value_cache": value_cache, "out_weight": out_weight, "final_gain": final_gain}


def layer_norm(values_in, gain_vec):
    row_mean = lax.optimization_barrier(jnp.mean(values_in, axis=-1, keepdims=True))
    centred = values_in - row_mean
    row_var = lax.optimization_barrier(jnp.mean(centred * centred, axis=-1, keepdims=True))
    return gain_vec * centred * lax.rsqrt(row_var + 1e-05)

def reference(token_ids, cache_lengths, embedding, ln_gain, query_weight, key_cache, value_cache, out_weight, final_gain):
    embedded = embedding[token_ids].astype(jnp.float32)
    normed = layer_norm(embedded, ln_gain).astype(jnp.bfloat16)
    queries = (jnp.dot(normed, query_weight, preferred_element_type=jnp.float32) * HD ** (-0.5)).astype(jnp.bfloat16)

    def attend_one(operands):
        query_row, key_rows, value_rows, length = operands
        head_query = query_row.reshape(HEADS, HD).astype(jnp.float32)
        key_heads = key_rows.reshape(CACHE, HEADS, HD).astype(jnp.float32)
        value_heads = value_rows.reshape(CACHE, HEADS, HD).astype(jnp.float32)
        scores = jnp.einsum('hd,thd->ht', head_query, key_heads)
        live_mask = jnp.arange(CACHE).astype(jnp.int32) < length
        scores = jnp.where(live_mask[None, :], scores, jnp.float32(-1e+30))
        row_top = lax.optimization_barrier(jnp.max(scores, axis=-1, keepdims=True))
        exp_terms = jnp.exp(scores - row_top)
        weights = (exp_terms / lax.optimization_barrier(jnp.sum(exp_terms, axis=-1, keepdims=True))).astype(jnp.bfloat16)
        result = jnp.einsum('ht,thd->hd', weights.astype(jnp.float32), value_heads)
        return result.reshape(HQ).astype(jnp.bfloat16)
    attended = lax.map(attend_one, (queries, key_cache, value_cache, cache_lengths))
    hidden = embedded + jnp.dot(attended, out_weight, preferred_element_type=jnp.float32)
    final_normed = layer_norm(hidden, final_gain).astype(jnp.bfloat16)
    logits = jnp.dot(final_normed, embedding.T, preferred_element_type=jnp.float32)
    return jax.nn.log_softmax(logits, axis=-1)
```

```python
import functools

import jax
import jax.numpy as jnp
from jax import lax
from jax.experimental import pallas as pl
from jax.experimental.pallas import tpu as pltpu
from jax.sharding import PartitionSpec as P

HD = 128
LANES = 128
EPS = 1e-05
MESH = pl.DeviceIdType.MESH
F32 = jnp.float32
BF16 = jnp.bfloat16


def to_lanes(column):
    rows = column.shape[0]
    row = lax.broadcasted_iota(jnp.int32, (rows, LANES), 0)
    lane = lax.broadcasted_iota(jnp.int32, (rows, LANES), 1)
    return jnp.sum(jnp.where(row == lane, column, 0.0), axis=0, keepdims=True)


def to_column(lanes, rows):
    row = lax.broadcasted_iota(jnp.int32, (rows, LANES), 0)
    lane = lax.broadcasted_iota(jnp.int32, (rows, LANES), 1)
    return jnp.sum(jnp.where(row == lane, lanes, 0.0), axis=1, keepdims=True)


def kernel(
    dp,
    mp,
    tokens,
    lengths,
    emb_hbm,
    ln_hbm,
    wq_hbm,
    key_hbm,
    val_hbm,
    wo_hbm,
    fg_hbm,
    out,
    emb,
    ln_gain,
    wq,
    keys,
    vals,
    wo,
    fin_gain,
    emb_send,
    emb_recv,
    emb_z,
    stat1,
    embedded,
    q_part,
    q_recv,
    att,
    o_part,
    o_recv,
    hid,
    stat2,
    fin,
    top,
    load_sem,
    emb_s,
    emb_r,
    z_s,
    z_r,
    st1_s,
    st1_r,
    q_s,
    q_r,
    att_s,
    att_r,
    o_s,
    o_r,
    hid_s,
    hid_r,
    st2_s,
    st2_r,
    fin_s,
    fin_r,
    top_s,
    top_r,
):
    d = lax.axis_index("dp")
    m = lax.axis_index("mp")
    n = dp * mp
    me = d * mp + m
    voc, width = emb.shape
    cols = wo.shape[1]
    seqs = dp * keys.shape[0]
    seq_here = keys.shape[0]
    heads_cols = wq.shape[1]
    rows = seqs // mp

    def load(src, dst, index):
        return pltpu.make_async_copy(src, dst, load_sem.at[index])

    here = pl.ds(pl.multiple_of(d * cols, LANES), cols)
    loads = [
        load(emb_hbm, emb, 0),
        load(ln_hbm.at[here], ln_gain, 1),
        load(wq_hbm, wq, 2),
        load(key_hbm, keys, 3),
        load(val_hbm, vals, 4),
        load(wo_hbm, wo, 5),
        load(fg_hbm.at[here], fin_gain, 6),
    ]
    for copy in loads:
        copy.start()

    barrier = pltpu.get_barrier_semaphore()

    def greet(k, carry):
        other = lax.rem(me + k, n)
        pl.semaphore_signal(
            barrier, inc=1, device_id=(other // mp, lax.rem(other, mp)), device_id_type=MESH
        )
        return carry

    lax.fori_loop(1, n, greet, 0)

    def over_dp(src, dst, send, recv, k):
        other = lax.rem(d + k, dp)
        return pltpu.make_async_remote_copy(
            src_ref=src(other),
            dst_ref=dst.at[d],
            send_sem=send.at[other],
            recv_sem=recv.at[d],
            device_id=(other, m),
            device_id_type=MESH,
        )

    def from_dp(dst, send, recv, k):
        other = lax.rem(d + k, dp)
        return pltpu.make_async_remote_copy(
            src_ref=dst.at[other],
            dst_ref=dst.at[other],
            send_sem=send.at[other],
            recv_sem=recv.at[other],
            device_id=(other, m),
            device_id_type=MESH,
        )

    def over_mp(src, dst, send, recv, k):
        other = lax.rem(m + k, mp)
        return pltpu.make_async_remote_copy(
            src_ref=src(other),
            dst_ref=dst.at[m],
            send_sem=send.at[other],
            recv_sem=recv.at[m],
            device_id=(d, other),
            device_id_type=MESH,
        )

    def from_mp(dst, send, recv, k):
        other = lax.rem(m + k, mp)
        return pltpu.make_async_remote_copy(
            src_ref=dst.at[other],
            dst_ref=dst.at[other],
            send_sem=send.at[other],
            recv_sem=recv.at[other],
            device_id=(d, other),
            device_id_type=MESH,
        )

    def small(buf, send, recv, other, slot):
        return pltpu.make_async_remote_copy(
            src_ref=buf.at[slot],
            dst_ref=buf.at[slot],
            send_sem=send.at[other],
            recv_sem=recv.at[slot],
            device_id=(other // mp, lax.rem(other, mp)),
            device_id_type=MESH,
        )

    def send_small(buf, send, recv):
        def body(k, carry):
            small(buf, send, recv, lax.rem(me + k, n), me).start()
            return carry

        lax.fori_loop(1, n, body, 0)

    def wait_small(buf, send, recv):
        def body(k, carry):
            other = lax.rem(me + k, n)
            small(buf, send, recv, other, other).wait_recv()
            return carry

        lax.fori_loop(1, n, body, 0)

    def sent_small(buf, send, recv):
        def body(k, carry):
            small(buf, send, recv, lax.rem(me + k, n), me).wait_send()
            return carry

        lax.fori_loop(1, n, body, 0)

    row = lax.broadcasted_iota(jnp.int32, (seqs, voc), 0)
    token = jnp.zeros((seqs, voc), jnp.int32)
    for s in range(seqs):
        token = jnp.where(row == s, tokens[s], token)
    voc_id = lax.broadcasted_iota(jnp.int32, (seqs, voc), 1) + me * voc
    one_hot = jnp.where(token == voc_id, 1.0, 0.0).astype(BF16)
    loads[0].wait()
    total = jnp.zeros((seqs, 1), F32)
    for j in range(dp):
        block = jnp.dot(
            one_hot, emb[:, j * cols : (j + 1) * cols], preferred_element_type=F32
        )
        emb_send[j] = block.astype(BF16)
        total = total + jnp.sum(block, axis=1, keepdims=True)
    pl.semaphore_wait(barrier, n - 1)
    sends = [over_dp(lambda j: emb_send.at[j], emb_recv, emb_s, emb_r, k) for k in range(1, dp)]
    for copy in sends:
        copy.start()
    mean = total * (1.0 / width)
    var = jnp.zeros((seqs, 1), F32)
    for j in range(dp):
        off = emb_send[j].astype(F32) - mean
        var = var + jnp.sum(off * off, axis=1, keepdims=True)
    stat1[me] = jnp.concatenate([to_lanes(mean), to_lanes(var * (1.0 / width))], axis=0)
    send_small(stat1, st1_s, st1_r)

    block_sum = emb_send[d].astype(F32)
    for k in range(1, dp):
        from_dp(emb_recv, emb_s, emb_r, k).wait_recv()
        block_sum = block_sum + emb_recv[lax.rem(d + k, dp)].astype(F32)
    emb_z[m] = block_sum.astype(BF16)
    z_sends = [over_mp(lambda j: emb_z.at[m], emb_z, z_s, z_r, k) for k in range(1, mp)]
    for copy in z_sends:
        copy.start()
    for copy in loads[1:]:
        copy.wait()
    wait_small(stat1, st1_s, st1_r)
    stats = jnp.sum(stat1[...], axis=0)
    first_mean = to_column(stats[0:1], seqs)
    first_scale = lax.rsqrt(to_column(stats[1:2], seqs) + EPS)
    for k in range(1, mp):
        from_mp(emb_z, z_s, z_r, k).wait_recv()
        block_sum = block_sum + emb_z[lax.rem(m + k, mp)].astype(F32)
    for j in range(mp):
        embedded[j] = block_sum[j * rows : (j + 1) * rows]

    gain = ln_gain[...].reshape(1, cols)
    normed = (gain * (block_sum - first_mean) * first_scale).astype(BF16)
    part = jnp.dot(normed, wq[...], preferred_element_type=F32)
    for j in range(dp):
        q_part[j] = part[j * seq_here : (j + 1) * seq_here]
    q_sends = [over_dp(lambda j: q_part.at[j], q_recv, q_s, q_r, k) for k in range(1, dp)]
    for copy in q_sends:
        copy.start()
    query_sum = q_part[d]
    for k in range(1, dp):
        from_dp(q_recv, q_s, q_r, k).wait_recv()
        query_sum = query_sum + q_recv[lax.rem(d + k, dp)]
    queries = (query_sum * HD ** (-0.5)).astype(BF16).astype(F32)

    heads = heads_cols // HD
    head_rows = -(-heads // 16) * 16
    cache_len = keys.shape[1]
    head_row = lax.broadcasted_iota(jnp.int32, (head_rows, heads_cols), 0)
    head_col = lax.broadcasted_iota(jnp.int32, (head_rows, heads_cols), 1)
    start = head_row * HD
    diagonal = (head_col >= start) & (head_col < start + HD)
    place = lax.broadcasted_iota(jnp.int32, (head_rows, cache_len), 1)
    rows_out = []
    for s in range(seq_here):
        spread = jnp.where(diagonal, queries[s : s + 1], 0.0).astype(BF16)
        scores = lax.dot_general(
            spread, keys[s], (((1,), (1,)), ((), ())), preferred_element_type=F32
        )
        scores = jnp.where(place < lengths[s], scores, F32(-1e30))
        exp_terms = jnp.exp(scores - jnp.max(scores, axis=-1, keepdims=True))
        weights = (exp_terms / jnp.sum(exp_terms, axis=-1, keepdims=True)).astype(BF16)
        mixed = jnp.dot(weights, vals[s], preferred_element_type=F32)
        rows_out.append(jnp.sum(jnp.where(diagonal, mixed, 0.0), axis=0, keepdims=True))
    att[d] = jnp.concatenate(rows_out, axis=0).astype(BF16)
    att_sends = [over_dp(lambda j: att.at[d], att, att_s, att_r, k) for k in range(1, dp)]
    for copy in att_sends:
        copy.start()
    for k in range(1, dp):
        from_dp(att, att_s, att_r, k).wait_recv()
    every = jnp.concatenate([att[j].astype(F32) for j in range(dp)], axis=0).astype(BF16)

    part = jnp.dot(every, wo[...], preferred_element_type=F32)
    for j in range(mp):
        o_part[j] = part[j * rows : (j + 1) * rows]
    o_sends = [over_mp(lambda j: o_part.at[j], o_recv, o_s, o_r, k) for k in range(1, mp)]
    for copy in o_sends:
        copy.start()
    mixed = o_part[m]
    for k in range(1, mp):
        from_mp(o_recv, o_s, o_r, k).wait_recv()
        mixed = mixed + o_recv[lax.rem(m + k, mp)]
    hidden = embedded[m] + mixed
    hid[m] = hidden
    hid_sends = [over_mp(lambda j: hid.at[m], hid, hid_s, hid_r, k) for k in range(1, mp)]
    for copy in hid_sends:
        copy.start()
    stat2[me] = jnp.concatenate(
        [
            to_lanes(jnp.sum(hidden, axis=1, keepdims=True)),
            to_lanes(jnp.sum(hidden * hidden, axis=1, keepdims=True)),
        ],
        axis=0,
    )
    send_small(stat2, st2_s, st2_r)
    for k in range(1, mp):
        from_mp(hid, hid_s, hid_r, k).wait_recv()
    wait_small(stat2, st2_s, st2_r)
    gain = fin_gain[...].reshape(1, cols)
    pieces = []
    for j in range(mp):
        stats = stat2[j]
        for i in range(1, dp):
            stats = stats + stat2[i * mp + j]
        stats = stats * (1.0 / width)
        row_mean = to_column(stats[0:1], rows)
        row_var = to_column(stats[1:2], rows) - row_mean * row_mean
        pieces.append(gain * (hid[j] - row_mean) * lax.rsqrt(row_var + EPS))
    fin[d] = jnp.concatenate(pieces, axis=0).astype(BF16)
    fin_sends = [over_dp(lambda j: fin.at[d], fin, fin_s, fin_r, k) for k in range(1, dp)]
    for copy in fin_sends:
        copy.start()

    def block_logits(j):
        features = pl.ds(pl.multiple_of(j * cols, LANES), cols)
        return lax.dot_general(
            fin[j], emb[:, features], (((1,), (1,)), ((), ())), preferred_element_type=F32
        )

    logits = block_logits(d)
    for k in range(1, dp):
        from_dp(fin, fin_s, fin_r, k).wait_recv()
        logits = logits + block_logits(lax.rem(d + k, dp))
    local_top = jnp.max(logits, axis=-1, keepdims=True)
    local_sum = jnp.sum(jnp.exp(logits - local_top), axis=-1, keepdims=True)
    top[me] = jnp.concatenate([to_lanes(local_top), to_lanes(local_sum)], axis=0)
    send_small(top, top_s, top_r)

    for copy in sends + z_sends + q_sends + att_sends + o_sends + hid_sends + fin_sends:
        copy.wait_send()
    sent_small(stat1, st1_s, st1_r)
    sent_small(stat2, st2_s, st2_r)
    wait_small(top, top_s, top_r)
    tops = top[:, 0:1, :]
    global_top = jnp.max(tops, axis=0)
    global_sum = jnp.sum(top[:, 1:2, :] * jnp.exp(tops - global_top[None]), axis=0)
    top_col = to_column(global_top, seqs)
    sum_col = to_column(global_sum, seqs)
    out[...] = logits - top_col - jnp.log(sum_col)
    sent_small(top, top_s, top_r)


def per_device(
    dp,
    mp,
    token_ids,
    cache_lengths,
    embedding,
    ln_gain,
    query_weight,
    key_cache,
    value_cache,
    out_weight,
    final_gain,
):
    n = dp * mp
    seqs = token_ids.shape[0]
    seq_here = key_cache.shape[0]
    cols = out_weight.shape[1]
    head_cols = query_weight.shape[1]
    rows = seqs // mp
    any_space = pl.BlockSpec(memory_space=pl.ANY)
    smem = pl.BlockSpec(memory_space=pltpu.SMEM)
    dma = pltpu.SemaphoreType.DMA
    pairs = [dp, mp, n, dp, dp, mp, mp, n, dp, n]
    return pl.pallas_call(
        functools.partial(kernel, dp, mp),
        out_shape=jax.ShapeDtypeStruct((seqs, embedding.shape[0]), F32),
        in_specs=[smem, smem] + [any_space] * 7,
        out_specs=pl.BlockSpec(memory_space=pltpu.VMEM),
        scratch_shapes=[
            pltpu.VMEM(embedding.shape, BF16),
            pltpu.VMEM((cols,), F32),
            pltpu.VMEM(query_weight.shape, BF16),
            pltpu.VMEM(key_cache.shape, BF16),
            pltpu.VMEM(value_cache.shape, BF16),
            pltpu.VMEM(out_weight.shape, BF16),
            pltpu.VMEM((cols,), F32),
            pltpu.VMEM((dp, seqs, cols), BF16),
            pltpu.VMEM((dp, seqs, cols), BF16),
            pltpu.VMEM((mp, seqs, cols), BF16),
            pltpu.VMEM((n, 2, LANES), F32),
            pltpu.VMEM((mp, rows, cols), F32),
            pltpu.VMEM((dp, seq_here, head_cols), F32),
            pltpu.VMEM((dp, seq_here, head_cols), F32),
            pltpu.VMEM((dp, seq_here, head_cols), BF16),
            pltpu.VMEM((mp, rows, cols), F32),
            pltpu.VMEM((mp, rows, cols), F32),
            pltpu.VMEM((mp, rows, cols), F32),
            pltpu.VMEM((n, 2, LANES), F32),
            pltpu.VMEM((dp, seqs, cols), BF16),
            pltpu.VMEM((n, 2, LANES), F32),
            dma((7,)),
        ]
        + [dma((size,)) for size in pairs for _ in range(2)],
        compiler_params=pltpu.CompilerParams(
            collective_id=0, has_side_effects=True, vmem_limit_bytes=60 * 1024 * 1024
        ),
    )(
        token_ids,
        cache_lengths,
        embedding,
        ln_gain,
        query_weight,
        key_cache,
        value_cache,
        out_weight,
        final_gain,
    )


def solution(mesh):
    return jax.shard_map(
        functools.partial(per_device, mesh.shape["dp"], mesh.shape["mp"]),
        mesh=mesh,
        in_specs=(
            P(),
            P("dp"),
            P(("dp", "mp"), None),
            P(),
            P("dp", "mp"),
            P("dp", None, "mp"),
            P("dp", None, "mp"),
            P("mp", "dp"),
            P(),
        ),
        out_specs=P(None, ("dp", "mp")),
        check_vma=False,
    )
```

```python
import functools

import jax
import jax.numpy as jnp
from jax import lax
from jax.experimental import pallas as pl
from jax.experimental.pallas import tpu as pltpu
from jax.sharding import PartitionSpec as P

HD = 128
LANES = 128
CHUNKS = 3
EPS = 1e-05
MESH = pl.DeviceIdType.MESH
F32 = jnp.float32
BF16 = jnp.bfloat16


def to_lanes(column):
    rows = column.shape[0]
    row = lax.broadcasted_iota(jnp.int32, (rows, LANES), 0)
    lane = lax.broadcasted_iota(jnp.int32, (rows, LANES), 1)
    return jnp.sum(jnp.where(row == lane, column, 0.0), axis=0, keepdims=True)


def to_column(lanes, rows):
    row = lax.broadcasted_iota(jnp.int32, (rows, LANES), 0)
    lane = lax.broadcasted_iota(jnp.int32, (rows, LANES), 1)
    return jnp.sum(jnp.where(row == lane, lanes, 0.0), axis=1, keepdims=True)


def kernel(
    dp,
    mp,
    tokens,
    lengths,
    emb_hbm,
    ln_hbm,
    wq_hbm,
    key_hbm,
    val_hbm,
    wo_hbm,
    fg_hbm,
    out,
    emb,
    ln_gain,
    wq,
    keys,
    vals,
    wo,
    fin_gain,
    emb_send,
    emb_recv,
    emb_z,
    stat1,
    embedded,
    q_part,
    q_recv,
    att,
    o_part,
    o_recv,
    hid,
    stat2,
    fin,
    top,
    hop,
    met,
    load_sem,
    emb_s,
    emb_r,
    z_s,
    z_r,
    st1_s,
    st1_r,
    q_s,
    q_r,
    att_s,
    att_r,
    o_s,
    o_r,
    hid_s,
    hid_r,
    st2_s,
    st2_r,
    fin_s,
    fin_r,
    top_s,
    top_r,
):
    d = lax.axis_index("dp")
    m = lax.axis_index("mp")
    n = dp * mp
    me = d * mp + m
    voc, width = emb.shape
    cols = wo.shape[1]
    seqs = dp * keys.shape[0]
    seq_here = keys.shape[0]
    heads_cols = wq.shape[1]
    rows = seqs // mp

    def load(src, dst, index):
        return pltpu.make_async_copy(src, dst, load_sem.at[index])

    here = pl.ds(pl.multiple_of(d * cols, LANES), cols)
    loads = [
        load(emb_hbm, emb, 0),
        load(ln_hbm.at[here], ln_gain, 1),
        load(wq_hbm, wq, 2),
        load(key_hbm, keys, 3),
        load(val_hbm, vals, 4),
        load(wo_hbm, wo, 5),
        load(fg_hbm.at[here], fin_gain, 6),
    ]
    for copy in loads:
        copy.start()

    barrier = pltpu.get_barrier_semaphore()

    def signal(sem, row, column):
        pl.semaphore_signal(sem, inc=1, device_id=(row, column), device_id_type=MESH)

    def signal_line(sem):
        @pl.when(m > 0)
        def _():
            signal(sem, d, m - 1)

        @pl.when(m < mp - 1)
        def _():
            signal(sem, d, m + 1)

    line = jnp.where(m > 0, 1, 0) + jnp.where(m < mp - 1, 1, 0)
    for k in range(1, dp):
        signal(barrier, lax.rem(d + k, dp), m)
    signal_line(barrier)

    def over_dp(src, dst, send, recv, k):
        other = lax.rem(d + k, dp)
        return pltpu.make_async_remote_copy(
            src_ref=src(other),
            dst_ref=dst.at[d],
            send_sem=send.at[other],
            recv_sem=recv.at[d],
            device_id=(other, m),
            device_id_type=MESH,
        )

    def from_dp(dst, send, recv, k):
        other = lax.rem(d + k, dp)
        return pltpu.make_async_remote_copy(
            src_ref=dst.at[other],
            dst_ref=dst.at[other],
            send_sem=send.at[other],
            recv_sem=recv.at[other],
            device_id=(other, m),
            device_id_type=MESH,
        )

    def over_mp(src, dst, send, recv, k):
        other = lax.rem(m + k, mp)
        return pltpu.make_async_remote_copy(
            src_ref=src(other),
            dst_ref=dst.at[m],
            send_sem=send.at[other],
            recv_sem=recv.at[m],
            device_id=(d, other),
            device_id_type=MESH,
        )

    def from_mp(dst, send, recv, k):
        other = lax.rem(m + k, mp)
        return pltpu.make_async_remote_copy(
            src_ref=dst.at[other],
            dst_ref=dst.at[other],
            send_sem=send.at[other],
            recv_sem=recv.at[other],
            device_id=(d, other),
            device_id_type=MESH,
        )

    def small(buf, send, recv, other, slot):
        return pltpu.make_async_remote_copy(
            src_ref=buf.at[slot],
            dst_ref=buf.at[slot],
            send_sem=send.at[other],
            recv_sem=recv.at[slot],
            device_id=(other // mp, lax.rem(other, mp)),
            device_id_type=MESH,
        )

    def send_small(buf, send, recv):
        def body(k, carry):
            small(buf, send, recv, lax.rem(me + k, n), me).start()
            return carry

        lax.fori_loop(1, n, body, 0)

    def wait_small(buf, send, recv):
        def body(k, carry):
            other = lax.rem(me + k, n)
            small(buf, send, recv, other, other).wait_recv()
            return carry

        lax.fori_loop(1, n, body, 0)

    def sent_small(buf, send, recv):
        def body(k, carry):
            small(buf, send, recv, lax.rem(me + k, n), me).wait_send()
            return carry

        lax.fori_loop(1, n, body, 0)

    row = lax.broadcasted_iota(jnp.int32, (seqs, voc), 0)
    token = jnp.zeros((seqs, voc), jnp.int32)
    for s in range(seqs):
        token = jnp.where(row == s, tokens[s], token)
    voc_id = lax.broadcasted_iota(jnp.int32, (seqs, voc), 1) + me * voc
    one_hot = jnp.where(token == voc_id, 1.0, 0.0).astype(BF16)
    loads[0].wait()
    chunks = emb_send.shape[0]
    wide = cols // chunks
    total = jnp.zeros((seqs, 1), F32)
    for i in range(chunks):
        for j in range(dp):
            begin = j * cols + i * wide
            block = jnp.dot(
                one_hot, emb[:, begin : begin + wide], preferred_element_type=F32
            )
            emb_send[i, j] = block.astype(BF16)
            total = total + jnp.sum(block, axis=1, keepdims=True)
    pl.semaphore_wait(barrier, dp - 1 + line)
    if mp > 2:
        signal_line(hop.at[0])
    sends = [
        over_dp(lambda j: emb_send.at[i, j], emb_recv.at[i], emb_s.at[i], emb_r.at[i], k)
        for i in range(chunks)
        for k in range(1, dp)
    ]
    for copy in sends:
        copy.start()
    mean = total * (1.0 / width)
    var = jnp.zeros((seqs, 1), F32)
    for i in range(chunks):
        for j in range(dp):
            off = emb_send[i, j].astype(F32) - mean
            var = var + jnp.sum(off * off, axis=1, keepdims=True)
    stat1[me] = jnp.concatenate([to_lanes(mean), to_lanes(var * (1.0 / width))], axis=0)
    for step in range(mp - 2):
        pl.semaphore_wait(hop.at[step], line)
        if step + 1 < mp - 2:
            signal_line(hop.at[step + 1])
    for k in range(1, dp):
        signal(met, lax.rem(d + k, dp), m)

    block_sums = []
    z_sends = []
    for i in range(chunks):
        part_sum = emb_send[i, d].astype(F32)
        for k in range(1, dp):
            from_dp(emb_recv.at[i], emb_s.at[i], emb_r.at[i], k).wait_recv()
            part_sum = part_sum + emb_recv[i, lax.rem(d + k, dp)].astype(F32)
        emb_z[i, m] = part_sum.astype(BF16)
        block_sums.append(part_sum)
        for k in range(1, mp):
            copy = over_mp(lambda j: emb_z.at[i, m], emb_z.at[i], z_s.at[i], z_r.at[i], k)
            copy.start()
            z_sends.append(copy)
        if i == 0:
            pl.semaphore_wait(met, dp - 1)
            send_small(stat1, st1_s, st1_r)
    for copy in loads[1:]:
        copy.wait()
    for i in range(chunks):
        for k in range(1, mp):
            from_mp(emb_z.at[i], z_s.at[i], z_r.at[i], k).wait_recv()
            block_sums[i] = block_sums[i] + emb_z[i, lax.rem(m + k, mp)].astype(F32)
    block_sum = jnp.concatenate(block_sums, axis=1)
    for j in range(mp):
        embedded[j] = block_sum[j * rows : (j + 1) * rows]
    wait_small(stat1, st1_s, st1_r)
    stats = jnp.sum(stat1[...], axis=0)
    first_mean = to_column(stats[0:1], seqs)
    first_scale = lax.rsqrt(to_column(stats[1:2], seqs) + EPS)

    gain = ln_gain[...].reshape(1, cols)
    normed = (gain * (block_sum - first_mean) * first_scale).astype(BF16)
    part = jnp.dot(normed, wq[...], preferred_element_type=F32)
    for j in range(dp):
        q_part[j] = part[j * seq_here : (j + 1) * seq_here]
    q_sends = [over_dp(lambda j: q_part.at[j], q_recv, q_s, q_r, k) for k in range(1, dp)]
    for copy in q_sends:
        copy.start()
    query_sum = q_part[d]
    for k in range(1, dp):
        from_dp(q_recv, q_s, q_r, k).wait_recv()
        query_sum = query_sum + q_recv[lax.rem(d + k, dp)]
    queries = (query_sum * HD ** (-0.5)).astype(BF16).astype(F32)

    heads = heads_cols // HD
    head_rows = -(-heads // 16) * 16
    cache_len = keys.shape[1]
    head_row = lax.broadcasted_iota(jnp.int32, (head_rows, heads_cols), 0)
    head_col = lax.broadcasted_iota(jnp.int32, (head_rows, heads_cols), 1)
    start = head_row * HD
    diagonal = (head_col >= start) & (head_col < start + HD)
    place = lax.broadcasted_iota(jnp.int32, (head_rows, cache_len), 1)
    rows_out = []
    for s in range(seq_here):
        spread = jnp.where(diagonal, queries[s : s + 1], 0.0).astype(BF16)
        scores = lax.dot_general(
            spread, keys[s], (((1,), (1,)), ((), ())), preferred_element_type=F32
        )
        scores = jnp.where(place < lengths[s], scores, F32(-1e30))
        exp_terms = jnp.exp(scores - jnp.max(scores, axis=-1, keepdims=True))
        weights = (exp_terms / jnp.sum(exp_terms, axis=-1, keepdims=True)).astype(BF16)
        mixed = jnp.dot(weights, vals[s], preferred_element_type=F32)
        rows_out.append(jnp.sum(jnp.where(diagonal, mixed, 0.0), axis=0, keepdims=True))
    att[d] = jnp.concatenate(rows_out, axis=0).astype(BF16)
    att_sends = [over_dp(lambda j: att.at[d], att, att_s, att_r, k) for k in range(1, dp)]
    for copy in att_sends:
        copy.start()
    for k in range(1, dp):
        from_dp(att, att_s, att_r, k).wait_recv()
    every = jnp.concatenate([att[j].astype(F32) for j in range(dp)], axis=0).astype(BF16)

    part = jnp.dot(every, wo[...], preferred_element_type=F32)
    for j in range(mp):
        o_part[j] = part[j * rows : (j + 1) * rows]
    o_sends = [over_mp(lambda j: o_part.at[j], o_recv, o_s, o_r, k) for k in range(1, mp)]
    for copy in o_sends:
        copy.start()
    mixed = o_part[m]
    for k in range(1, mp):
        from_mp(o_recv, o_s, o_r, k).wait_recv()
        mixed = mixed + o_recv[lax.rem(m + k, mp)]
    hidden = embedded[m] + mixed
    hid[m] = hidden
    hid_sends = [over_mp(lambda j: hid.at[m], hid, hid_s, hid_r, k) for k in range(1, mp)]
    for copy in hid_sends:
        copy.start()
    stat2[me] = jnp.concatenate(
        [
            to_lanes(jnp.sum(hidden, axis=1, keepdims=True)),
            to_lanes(jnp.sum(hidden * hidden, axis=1, keepdims=True)),
        ],
        axis=0,
    )
    send_small(stat2, st2_s, st2_r)
    for k in range(1, mp):
        from_mp(hid, hid_s, hid_r, k).wait_recv()
    wait_small(stat2, st2_s, st2_r)
    gain = fin_gain[...].reshape(1, cols)
    pieces = []
    for j in range(mp):
        stats = stat2[j]
        for i in range(1, dp):
            stats = stats + stat2[i * mp + j]
        stats = stats * (1.0 / width)
        row_mean = to_column(stats[0:1], rows)
        row_var = to_column(stats[1:2], rows) - row_mean * row_mean
        pieces.append(gain * (hid[j] - row_mean) * lax.rsqrt(row_var + EPS))
    fin[d] = jnp.concatenate(pieces, axis=0).astype(BF16)
    core = lax.rem(d, 2)
    chip = d // 2
    partner = d + 1 - 2 * core
    swap = 1 - 2 * core

    def fin_copy(slot, target, index):
        return pltpu.make_async_remote_copy(
            src_ref=fin.at[slot],
            dst_ref=fin.at[slot],
            send_sem=fin_s.at[index],
            recv_sem=fin_r.at[slot],
            device_id=(target, m),
            device_id_type=MESH,
        )

    others = [2 * lax.rem(chip + k, dp // 2) + core for k in range(1, dp // 2)]
    fin_sends = [fin_copy(d, other, other) for other in others] + [fin_copy(d, partner, partner)]
    for copy in fin_sends:
        copy.start()

    def block_logits(j):
        features = pl.ds(pl.multiple_of(j * cols, LANES), cols)
        return lax.dot_general(
            fin[j], emb[:, features], (((1,), (1,)), ((), ())), preferred_element_type=F32
        )

    logits = block_logits(d)
    fin_copy(partner, partner, partner).wait_recv()
    logits = logits + block_logits(partner)
    for other in others:
        fin_copy(other, other, other).wait_recv()
        passed = fin_copy(other, partner, other + swap)
        passed.start()
        fin_sends.append(passed)
        logits = logits + block_logits(other)
    for other in others:
        fin_copy(other + swap, partner, partner).wait_recv()
        logits = logits + block_logits(other + swap)
    local_top = jnp.max(logits, axis=-1, keepdims=True)
    local_sum = jnp.sum(jnp.exp(logits - local_top), axis=-1, keepdims=True)
    top[me] = jnp.concatenate([to_lanes(local_top), to_lanes(local_sum)], axis=0)
    send_small(top, top_s, top_r)

    for copy in sends + z_sends + q_sends + att_sends + o_sends + hid_sends + fin_sends:
        copy.wait_send()
    sent_small(stat1, st1_s, st1_r)
    sent_small(stat2, st2_s, st2_r)
    wait_small(top, top_s, top_r)
    tops = top[:, 0:1, :]
    global_top = jnp.max(tops, axis=0)
    global_sum = jnp.sum(top[:, 1:2, :] * jnp.exp(tops - global_top[None]), axis=0)
    top_col = to_column(global_top, seqs)
    sum_col = to_column(global_sum, seqs)
    out[...] = logits - top_col - jnp.log(sum_col)
    sent_small(top, top_s, top_r)


def per_device(
    dp,
    mp,
    token_ids,
    cache_lengths,
    embedding,
    ln_gain,
    query_weight,
    key_cache,
    value_cache,
    out_weight,
    final_gain,
):
    n = dp * mp
    seqs = token_ids.shape[0]
    seq_here = key_cache.shape[0]
    cols = out_weight.shape[1]
    head_cols = query_weight.shape[1]
    rows = seqs // mp
    chunks = next(k for k in (CHUNKS, 2, 1) if cols % (k * LANES) == 0)
    wide = cols // chunks
    any_space = pl.BlockSpec(memory_space=pl.ANY)
    smem = pl.BlockSpec(memory_space=pltpu.SMEM)
    dma = pltpu.SemaphoreType.DMA
    pairs = [(chunks, dp), (chunks, mp)] + [(k,) for k in (n, dp, dp, mp, mp, n, dp, n)]
    return pl.pallas_call(
        functools.partial(kernel, dp, mp),
        out_shape=jax.ShapeDtypeStruct((seqs, embedding.shape[0]), F32),
        in_specs=[smem, smem] + [any_space] * 7,
        out_specs=pl.BlockSpec(memory_space=pltpu.VMEM),
        scratch_shapes=[
            pltpu.VMEM(embedding.shape, BF16),
            pltpu.VMEM((cols,), F32),
            pltpu.VMEM(query_weight.shape, BF16),
            pltpu.VMEM(key_cache.shape, BF16),
            pltpu.VMEM(value_cache.shape, BF16),
            pltpu.VMEM(out_weight.shape, BF16),
            pltpu.VMEM((cols,), F32),
            pltpu.VMEM((chunks, dp, seqs, wide), BF16),
            pltpu.VMEM((chunks, dp, seqs, wide), BF16),
            pltpu.VMEM((chunks, mp, seqs, wide), BF16),
            pltpu.VMEM((n, 2, LANES), F32),
            pltpu.VMEM((mp, rows, cols), F32),
            pltpu.VMEM((dp, seq_here, head_cols), F32),
            pltpu.VMEM((dp, seq_here, head_cols), F32),
            pltpu.VMEM((dp, seq_here, head_cols), BF16),
            pltpu.VMEM((mp, rows, cols), F32),
            pltpu.VMEM((mp, rows, cols), F32),
            pltpu.VMEM((mp, rows, cols), F32),
            pltpu.VMEM((n, 2, LANES), F32),
            pltpu.VMEM((dp, seqs, cols), BF16),
            pltpu.VMEM((n, 2, LANES), F32),
            pltpu.SemaphoreType.REGULAR((max(mp - 2, 1),)),
            pltpu.SemaphoreType.REGULAR,
            dma((7,)),
        ]
        + [dma(size) for size in pairs for _ in range(2)],
        compiler_params=pltpu.CompilerParams(
            collective_id=0, has_side_effects=True, vmem_limit_bytes=60 * 1024 * 1024
        ),
    )(
        token_ids,
        cache_lengths,
        embedding,
        ln_gain,
        query_weight,
        key_cache,
        value_cache,
        out_weight,
        final_gain,
    )


def solution(mesh):
    return jax.shard_map(
        functools.partial(per_device, mesh.shape["dp"], mesh.shape["mp"]),
        mesh=mesh,
        in_specs=(
            P(),
            P("dp"),
            P(("dp", "mp"), None),
            P(),
            P("dp", "mp"),
            P("dp", None, "mp"),
            P("dp", None, "mp"),
            P("mp", "dp"),
            P(),
        ),
        out_specs=P(None, ("dp", "mp")),
        check_vma=False,
    )
```

```python
import functools

import jax
import jax.numpy as jnp
from jax import lax
from jax.experimental import pallas as pl
from jax.experimental.pallas import tpu as pltpu
from jax.sharding import PartitionSpec as P

HD = 128
LANES = 128
CHUNKS = 3
EPS = 1e-05
MESH = pl.DeviceIdType.MESH
F32 = jnp.float32
BF16 = jnp.bfloat16


def to_lanes(column):
    rows = column.shape[0]
    row = lax.broadcasted_iota(jnp.int32, (rows, LANES), 0)
    lane = lax.broadcasted_iota(jnp.int32, (rows, LANES), 1)
    return jnp.sum(jnp.where(row == lane, column, 0.0), axis=0, keepdims=True)


def to_column(lanes, rows):
    row = lax.broadcasted_iota(jnp.int32, (rows, LANES), 0)
    lane = lax.broadcasted_iota(jnp.int32, (rows, LANES), 1)
    return jnp.sum(jnp.where(row == lane, lanes, 0.0), axis=1, keepdims=True)


def kernel(
    dp,
    mp,
    tokens,
    lengths,
    emb_hbm,
    ln_hbm,
    wq_hbm,
    key_hbm,
    val_hbm,
    wo_hbm,
    fg_hbm,
    out,
    emb,
    ln_gain,
    wq,
    keys,
    vals,
    wo,
    fin_gain,
    emb_send,
    emb_recv,
    emb_z,
    stat1,
    embedded,
    q_part,
    q_recv,
    att,
    o_part,
    o_recv,
    hid,
    stat2,
    fin,
    top,
    hop,
    met,
    load_sem,
    emb_s,
    emb_r,
    z_s,
    z_r,
    st1_s,
    st1_r,
    q_s,
    q_r,
    att_s,
    att_r,
    o_s,
    o_r,
    hid_s,
    hid_r,
    st2_s,
    st2_r,
    fin_s,
    fin_r,
    top_s,
    top_r,
):
    d = lax.axis_index("dp")
    m = lax.axis_index("mp")
    n = dp * mp
    me = d * mp + m
    voc, width = emb.shape
    cols = wo.shape[1]
    seqs = dp * keys.shape[0]
    seq_here = keys.shape[0]
    heads_cols = wq.shape[1]
    rows = seqs // mp

    def load(src, dst, index):
        return pltpu.make_async_copy(src, dst, load_sem.at[index])

    here = pl.ds(pl.multiple_of(d * cols, LANES), cols)
    loads = [
        load(emb_hbm, emb, 0),
        load(ln_hbm.at[here], ln_gain, 1),
        load(wq_hbm, wq, 2),
        load(key_hbm, keys, 3),
        load(val_hbm, vals, 4),
        load(wo_hbm, wo, 5),
        load(fg_hbm.at[here], fin_gain, 6),
    ]
    for copy in loads:
        copy.start()

    barrier = pltpu.get_barrier_semaphore()

    def signal(sem, row, column):
        pl.semaphore_signal(sem, inc=1, device_id=(row, column), device_id_type=MESH)

    def signal_line(sem):
        @pl.when(m > 0)
        def _():
            signal(sem, d, m - 1)

        @pl.when(m < mp - 1)
        def _():
            signal(sem, d, m + 1)

    line = jnp.where(m > 0, 1, 0) + jnp.where(m < mp - 1, 1, 0)
    for k in range(1, dp):
        signal(barrier, lax.rem(d + k, dp), m)
    signal_line(barrier)

    core = lax.rem(d, 2)
    chip = d // 2
    chips = dp // 2
    partner = d + 1 - 2 * core
    swap = 1 - 2 * core
    corner = chips - 1 - chip
    own = lax.rem(chip - corner + chips, chips)
    chip_order = [lax.rem(corner + t + jnp.where(own <= t, 1, 0), chips) for t in range(chips - 1)]
    others = [2 * c + core for c in chip_order]
    far_dp = [j for other in others for j in (other, other + swap)] + [partner]
    near_dp = far_dp[::-1]
    upper = 2 * m >= mp
    far_mp = [
        jnp.where(
            upper,
            t + jnp.where(m <= t, 1, 0),
            mp - 1 - t - jnp.where(mp - 1 - m <= t, 1, 0),
        )
        for t in range(mp - 1)
    ]
    near_mp = far_mp[::-1]

    def over_dp(src, dst, send, recv, k):
        other = far_dp[k - 1]
        return pltpu.make_async_remote_copy(
            src_ref=src(other),
            dst_ref=dst.at[d],
            send_sem=send.at[other],
            recv_sem=recv.at[d],
            device_id=(other, m),
            device_id_type=MESH,
        )

    def from_dp(dst, send, recv, k):
        other = near_dp[k - 1]
        return pltpu.make_async_remote_copy(
            src_ref=dst.at[other],
            dst_ref=dst.at[other],
            send_sem=send.at[other],
            recv_sem=recv.at[other],
            device_id=(other, m),
            device_id_type=MESH,
        )

    def over_mp(src, dst, send, recv, k):
        other = far_mp[k - 1]
        return pltpu.make_async_remote_copy(
            src_ref=src(other),
            dst_ref=dst.at[m],
            send_sem=send.at[other],
            recv_sem=recv.at[m],
            device_id=(d, other),
            device_id_type=MESH,
        )

    def from_mp(dst, send, recv, k):
        other = near_mp[k - 1]
        return pltpu.make_async_remote_copy(
            src_ref=dst.at[other],
            dst_ref=dst.at[other],
            send_sem=send.at[other],
            recv_sem=recv.at[other],
            device_id=(d, other),
            device_id_type=MESH,
        )

    def small(buf, send, recv, other, slot):
        return pltpu.make_async_remote_copy(
            src_ref=buf.at[slot],
            dst_ref=buf.at[slot],
            send_sem=send.at[other],
            recv_sem=recv.at[slot],
            device_id=(other // mp, lax.rem(other, mp)),
            device_id_type=MESH,
        )

    def send_small(buf, send, recv):
        def body(k, carry):
            small(buf, send, recv, lax.rem(me + k, n), me).start()
            return carry

        lax.fori_loop(1, n, body, 0)

    def wait_small(buf, send, recv):
        def body(k, carry):
            other = lax.rem(me + k, n)
            small(buf, send, recv, other, other).wait_recv()
            return carry

        lax.fori_loop(1, n, body, 0)

    def sent_small(buf, send, recv):
        def body(k, carry):
            small(buf, send, recv, lax.rem(me + k, n), me).wait_send()
            return carry

        lax.fori_loop(1, n, body, 0)

    row = lax.broadcasted_iota(jnp.int32, (seqs, voc), 0)
    token = jnp.zeros((seqs, voc), jnp.int32)
    for s in range(seqs):
        token = jnp.where(row == s, tokens[s], token)
    voc_id = lax.broadcasted_iota(jnp.int32, (seqs, voc), 1) + me * voc
    one_hot = jnp.where(token == voc_id, 1.0, 0.0).astype(BF16)
    loads[0].wait()
    chunks = emb_send.shape[0]
    wide = cols // chunks
    total = jnp.zeros((seqs, 1), F32)
    for i in range(chunks):
        for j in range(dp):
            begin = j * cols + i * wide
            block = jnp.dot(
                one_hot, emb[:, begin : begin + wide], preferred_element_type=F32
            )
            emb_send[i, j] = block.astype(BF16)
            total = total + jnp.sum(block, axis=1, keepdims=True)
    pl.semaphore_wait(barrier, dp - 1 + line)
    if mp > 2:
        signal_line(hop.at[0])
    sends = [
        over_dp(lambda j: emb_send.at[i, j], emb_recv.at[i], emb_s.at[i], emb_r.at[i], k)
        for i in range(chunks)
        for k in range(1, dp)
    ]
    for copy in sends:
        copy.start()
    mean = total * (1.0 / width)
    var = jnp.zeros((seqs, 1), F32)
    for i in range(chunks):
        for j in range(dp):
            off = emb_send[i, j].astype(F32) - mean
            var = var + jnp.sum(off * off, axis=1, keepdims=True)
    stat1[me] = jnp.concatenate([to_lanes(mean), to_lanes(var * (1.0 / width))], axis=0)
    for step in range(mp - 2):
        pl.semaphore_wait(hop.at[step], line)
        if step + 1 < mp - 2:
            signal_line(hop.at[step + 1])
    for k in range(1, dp):
        signal(met, lax.rem(d + k, dp), m)

    block_sums = []
    z_sends = []
    for i in range(chunks):
        part_sum = emb_send[i, d].astype(F32)
        for k in range(1, dp):
            from_dp(emb_recv.at[i], emb_s.at[i], emb_r.at[i], k).wait_recv()
            part_sum = part_sum + emb_recv[i, near_dp[k - 1]].astype(F32)
        emb_z[i, m] = part_sum.astype(BF16)
        block_sums.append(part_sum)
        for k in range(1, mp):
            copy = over_mp(lambda j: emb_z.at[i, m], emb_z.at[i], z_s.at[i], z_r.at[i], k)
            copy.start()
            z_sends.append(copy)
        if i == 0:
            pl.semaphore_wait(met, dp - 1)
            send_small(stat1, st1_s, st1_r)
    for copy in loads[1:]:
        copy.wait()
    for i in range(chunks):
        for k in range(1, mp):
            from_mp(emb_z.at[i], z_s.at[i], z_r.at[i], k).wait_recv()
            block_sums[i] = block_sums[i] + emb_z[i, near_mp[k - 1]].astype(F32)
    block_sum = jnp.concatenate(block_sums, axis=1)
    for j in range(mp):
        embedded[j] = block_sum[j * rows : (j + 1) * rows]
    wait_small(stat1, st1_s, st1_r)
    stats = jnp.sum(stat1[...], axis=0)
    first_mean = to_column(stats[0:1], seqs)
    first_scale = lax.rsqrt(to_column(stats[1:2], seqs) + EPS)

    gain = ln_gain[...].reshape(1, cols)
    normed = (gain * (block_sum - first_mean) * first_scale).astype(BF16)
    part = jnp.dot(normed, wq[...], preferred_element_type=F32)
    for j in range(dp):
        q_part[j] = part[j * seq_here : (j + 1) * seq_here]
    q_sends = [over_dp(lambda j: q_part.at[j], q_recv, q_s, q_r, k) for k in range(1, dp)]
    for copy in q_sends:
        copy.start()
    query_sum = q_part[d]
    for k in range(1, dp):
        from_dp(q_recv, q_s, q_r, k).wait_recv()
        query_sum = query_sum + q_recv[near_dp[k - 1]]
    queries = (query_sum * HD ** (-0.5)).astype(BF16).astype(F32)

    heads = heads_cols // HD
    head_rows = -(-heads // 16) * 16
    cache_len = keys.shape[1]
    head_row = lax.broadcasted_iota(jnp.int32, (head_rows, heads_cols), 0)
    head_col = lax.broadcasted_iota(jnp.int32, (head_rows, heads_cols), 1)
    start = head_row * HD
    diagonal = (head_col >= start) & (head_col < start + HD)
    place = lax.broadcasted_iota(jnp.int32, (head_rows, cache_len), 1)
    rows_out = []
    for s in range(seq_here):
        spread = jnp.where(diagonal, queries[s : s + 1], 0.0).astype(BF16)
        scores = lax.dot_general(
            spread, keys[s], (((1,), (1,)), ((), ())), preferred_element_type=F32
        )
        scores = jnp.where(place < lengths[s], scores, F32(-1e30))
        exp_terms = jnp.exp(scores - jnp.max(scores, axis=-1, keepdims=True))
        weights = (exp_terms / jnp.sum(exp_terms, axis=-1, keepdims=True)).astype(BF16)
        mixed = jnp.dot(weights, vals[s], preferred_element_type=F32)
        rows_out.append(jnp.sum(jnp.where(diagonal, mixed, 0.0), axis=0, keepdims=True))
    att[d] = jnp.concatenate(rows_out, axis=0).astype(BF16)
    att_sends = [over_dp(lambda j: att.at[d], att, att_s, att_r, k) for k in range(1, dp)]
    for copy in att_sends:
        copy.start()
    for k in range(1, dp):
        from_dp(att, att_s, att_r, k).wait_recv()
    every = jnp.concatenate([att[j].astype(F32) for j in range(dp)], axis=0).astype(BF16)

    part = jnp.dot(every, wo[...], preferred_element_type=F32)
    for j in range(mp):
        o_part[j] = part[j * rows : (j + 1) * rows]
    o_sends = [over_mp(lambda j: o_part.at[j], o_recv, o_s, o_r, k) for k in range(1, mp)]
    for copy in o_sends:
        copy.start()
    mixed = o_part[m]
    for k in range(1, mp):
        from_mp(o_recv, o_s, o_r, k).wait_recv()
        mixed = mixed + o_recv[near_mp[k - 1]]
    hidden = embedded[m] + mixed
    hid[m] = hidden
    stat2[me] = jnp.concatenate(
        [
            to_lanes(jnp.sum(hidden, axis=1, keepdims=True)),
            to_lanes(jnp.sum(hidden * hidden, axis=1, keepdims=True)),
        ],
        axis=0,
    )
    send_small(stat2, st2_s, st2_r)
    hid_sends = [over_mp(lambda j: hid.at[m], hid, hid_s, hid_r, k) for k in range(1, mp)]
    for copy in hid_sends:
        copy.start()
    for k in range(1, mp):
        from_mp(hid, hid_s, hid_r, k).wait_recv()
    wait_small(stat2, st2_s, st2_r)
    gain = fin_gain[...].reshape(1, cols)
    pieces = []
    for j in range(mp):
        stats = stat2[j]
        for i in range(1, dp):
            stats = stats + stat2[i * mp + j]
        stats = stats * (1.0 / width)
        row_mean = to_column(stats[0:1], rows)
        row_var = to_column(stats[1:2], rows) - row_mean * row_mean
        pieces.append(gain * (hid[j] - row_mean) * lax.rsqrt(row_var + EPS))
    fin[d] = jnp.concatenate(pieces, axis=0).astype(BF16)
    def fin_copy(slot, target, index):
        return pltpu.make_async_remote_copy(
            src_ref=fin.at[slot],
            dst_ref=fin.at[slot],
            send_sem=fin_s.at[index],
            recv_sem=fin_r.at[slot],
            device_id=(target, m),
            device_id_type=MESH,
        )

    fin_sends = [fin_copy(d, other, other) for other in others] + [fin_copy(d, partner, partner)]
    for copy in fin_sends:
        copy.start()

    def block_logits(j):
        features = pl.ds(pl.multiple_of(j * cols, LANES), cols)
        return lax.dot_general(
            fin[j], emb[:, features], (((1,), (1,)), ((), ())), preferred_element_type=F32
        )

    logits = block_logits(d)
    fin_copy(partner, partner, partner).wait_recv()
    logits = logits + block_logits(partner)
    for other in others[::-1]:
        fin_copy(other, other, other).wait_recv()
        passed = fin_copy(other, partner, other + swap)
        passed.start()
        fin_sends.append(passed)
        logits = logits + block_logits(other)
    for other in others[::-1]:
        fin_copy(other + swap, partner, partner).wait_recv()
        logits = logits + block_logits(other + swap)
    local_top = jnp.max(logits, axis=-1, keepdims=True)
    local_sum = jnp.sum(jnp.exp(logits - local_top), axis=-1, keepdims=True)
    top[me] = jnp.concatenate([to_lanes(local_top), to_lanes(local_sum)], axis=0)
    send_small(top, top_s, top_r)

    for copy in sends + z_sends + q_sends + att_sends + o_sends + hid_sends + fin_sends:
        copy.wait_send()
    sent_small(stat1, st1_s, st1_r)
    sent_small(stat2, st2_s, st2_r)
    wait_small(top, top_s, top_r)
    tops = top[:, 0:1, :]
    global_top = jnp.max(tops, axis=0)
    global_sum = jnp.sum(top[:, 1:2, :] * jnp.exp(tops - global_top[None]), axis=0)
    top_col = to_column(global_top, seqs)
    sum_col = to_column(global_sum, seqs)
    out[...] = logits - top_col - jnp.log(sum_col)
    sent_small(top, top_s, top_r)


def per_device(
    dp,
    mp,
    token_ids,
    cache_lengths,
    embedding,
    ln_gain,
    query_weight,
    key_cache,
    value_cache,
    out_weight,
    final_gain,
):
    n = dp * mp
    seqs = token_ids.shape[0]
    seq_here = key_cache.shape[0]
    cols = out_weight.shape[1]
    head_cols = query_weight.shape[1]
    rows = seqs // mp
    chunks = next(k for k in (CHUNKS, 2, 1) if cols % (k * LANES) == 0)
    wide = cols // chunks
    any_space = pl.BlockSpec(memory_space=pl.ANY)
    smem = pl.BlockSpec(memory_space=pltpu.SMEM)
    dma = pltpu.SemaphoreType.DMA
    pairs = [(chunks, dp), (chunks, mp)] + [(k,) for k in (n, dp, dp, mp, mp, n, dp, n)]
    return pl.pallas_call(
        functools.partial(kernel, dp, mp),
        out_shape=jax.ShapeDtypeStruct((seqs, embedding.shape[0]), F32),
        in_specs=[smem, smem] + [any_space] * 7,
        out_specs=pl.BlockSpec(memory_space=pltpu.VMEM),
        scratch_shapes=[
            pltpu.VMEM(embedding.shape, BF16),
            pltpu.VMEM((cols,), F32),
            pltpu.VMEM(query_weight.shape, BF16),
            pltpu.VMEM(key_cache.shape, BF16),
            pltpu.VMEM(value_cache.shape, BF16),
            pltpu.VMEM(out_weight.shape, BF16),
            pltpu.VMEM((cols,), F32),
            pltpu.VMEM((chunks, dp, seqs, wide), BF16),
            pltpu.VMEM((chunks, dp, seqs, wide), BF16),
            pltpu.VMEM((chunks, mp, seqs, wide), BF16),
            pltpu.VMEM((n, 2, LANES), F32),
            pltpu.VMEM((mp, rows, cols), F32),
            pltpu.VMEM((dp, seq_here, head_cols), F32),
            pltpu.VMEM((dp, seq_here, head_cols), F32),
            pltpu.VMEM((dp, seq_here, head_cols), BF16),
            pltpu.VMEM((mp, rows, cols), F32),
            pltpu.VMEM((mp, rows, cols), F32),
            pltpu.VMEM((mp, rows, cols), F32),
            pltpu.VMEM((n, 2, LANES), F32),
            pltpu.VMEM((dp, seqs, cols), BF16),
            pltpu.VMEM((n, 2, LANES), F32),
            pltpu.SemaphoreType.REGULAR((max(mp - 2, 1),)),
            pltpu.SemaphoreType.REGULAR,
            dma((7,)),
        ]
        + [dma(size) for size in pairs for _ in range(2)],
        compiler_params=pltpu.CompilerParams(
            collective_id=0, has_side_effects=True, vmem_limit_bytes=60 * 1024 * 1024
        ),
    )(
        token_ids,
        cache_lengths,
        embedding,
        ln_gain,
        query_weight,
        key_cache,
        value_cache,
        out_weight,
        final_gain,
    )


def solution(mesh):
    return jax.shard_map(
        functools.partial(per_device, mesh.shape["dp"], mesh.shape["mp"]),
        mesh=mesh,
        in_specs=(
            P(),
            P("dp"),
            P(("dp", "mp"), None),
            P(),
            P("dp", "mp"),
            P("dp", None, "mp"),
            P("dp", None, "mp"),
            P("mp", "dp"),
            P(),
        ),
        out_specs=P(None, ("dp", "mp")),
        check_vma=False,
    )
```
